32 devices in a mesh: blk: 16 (over z, y, core), shard: 2 (over x).
Axes of the slice: x: 2, y: 2, z: 4, core: 2. Of those that a mesh axis runs over, the one named last changes fastest.
Arguments:
- cut_acts: bfloat16 [8192, 1024], P('blk'), may hold values from -6 to 6
- upstream: bfloat16 [8192, 1024], P('blk', 'shard'), may hold values from -1 to 1
- weights: bfloat16 [16, 1024, 1024], P('blk', None, 'shard'), may hold values from -0.59765625 to 0.59765625
- moment_one: float32 [16, 1024, 1024], P('blk', None, 'shard'), may hold values from -6 to 6
- moment_two: float32 [16, 1024, 1024], P('blk', None, 'shard'), may hold values from 1 to 8
Outputs:
- new_weights: bfloat16 [16, 1024, 1024], P('blk', None, 'shard')
- new_moment_one: float32 [16, 1024, 1024], P('blk', None, 'shard')
- new_moment_two: float32 [16, 1024, 1024], P('blk', None, 'shard')
- cut_grads: bfloat16 [3, 8192, 1024], P(None, ('blk', 'shard'))
The draws below stay inside these ranges and needn't reach their ends.
All inputs are finite; a program needn't handle non-finite values.
Results may differ from the reference program's by a relative error of at most 0.0074.
Values may be sent and summed in bfloat16 or wider, within the bound.
No kernel may reach another device: no remote copies, remote signals or barrier semaphores. Data moves between devices by JAX's collectives and lax.ppermute only.
A program may use at most 64 MiB of HBM per device.

```python
import math
import jax
import jax.numpy as jnp
from jax import lax

D = 1024
HOPS = 3
ROWS = 512
CLIENTS = 16
TOK_ALL = 8192
N_BLK = 16


def shard_levels(stream_key, dims, split, smallest, top_value):
    factor_of = 1.0
    for dim, shards_of in split:
        draws = jax.random.uniform(jax.random.fold_in(jax.random.fold_in(stream_key, 6), dim), (shards_of,), jnp.float32, smallest / len(split), top_value / len(split))
        factor_of = factor_of * jnp.repeat(jnp.exp(draws), dims[dim] // shards_of).reshape((-1,) + (1,) * (len(dims) - 1 - dim))
    return factor_of


def centred(own_key, dims, spread, most, split=(), dtype=jnp.bfloat16):
    level = shard_levels(own_key, dims, split, -0.22, 0.18) if split else 1.0
    entries = jax.random.normal(own_key, dims, jnp.float32) * spread * level
    return jnp.minimum(jnp.maximum(entries, -most), most).astype(dtype)


def setup_inputs(seed: int = 0) -> dict:
    streams_of = jax.random.split(jax.random.key(seed), 6)
    cut_acts = centred(streams_of[0], (TOK_ALL, D), 1.0, 6.0, ((0, 16),))
    upstream = centred(streams_of[1], (TOK_ALL, D), 0.125, 1.0, ((0, 16), (1, 2)))
    weights = centred(streams_of[2], (CLIENTS, D, D), 0.1, 0.59765625, ((0, 16), (2, 2)))
    moment_one = centred(streams_of[3], (CLIENTS, D, D), 1.0, 6.0, ((0, 16), (2, 2)), jnp.float32)
    moment_two = jnp.clip(jnp.exp(math.log(8.0) - 2.0794415 * jax.random.uniform(streams_of[4], (CLIENTS, D, D), jnp.float32) ** shard_levels(streams_of[4], (CLIENTS, D, D), ((0, 16), (2, 2)), -0.2, 0.2)), 1.0, 8.0)
    return {"cut_acts": cut_acts, "upstream": upstream, "weights": weights, "moment_one": moment_one, "moment_two": moment_two}


def gelu_slope(values):
    inner = 0.7978845608 * (values + 0.044715 * values * values * values)
    tanh_part = jnp.tanh(inner)
    return 0.5 * (1.0 + tanh_part) + 0.5 * values * (1.0 - tanh_part * tanh_part) * 0.7978845608 * (1.0 + 0.134145 * values * values)

def train_hop(operands):
    kernel, first, second, inputs, grad_out = operands
    preact = jnp.dot(inputs, kernel, preferred_element_type=jnp.float32)
    slopes = (grad_out.astype(jnp.float32) * gelu_slope(preact)).astype(jnp.bfloat16)
    gradient = jnp.dot(inputs.T, slopes, preferred_element_type=jnp.float32)
    returned = jnp.dot(slopes, kernel.T, preferred_element_type=jnp.float32).astype(jnp.bfloat16)
    first = 0.9 * first + 0.1 * gradient
    second = 0.95 * second + 0.05 * gradient * gradient
    kernel = (kernel.astype(jnp.float32) - 0.01 * first / (jnp.sqrt(second) + 1e-08)).astype(jnp.bfloat16)
    return (kernel, first, second, returned)

def reference(cut_acts, upstream, weights, moment_one, moment_two):
    acts_split = cut_acts.reshape(N_BLK, ROWS, D)
    grads_split = upstream.reshape(N_BLK, ROWS, D)
    kernel, first, second = (weights, moment_one, moment_two)
    returned_all = []
    for hop_index in range(HOPS):
        shifted_acts = jnp.roll(acts_split, -hop_index, axis=0)
        shifted_grads = jnp.roll(grads_split, -hop_index, axis=0)
        kernel, first, second, returned = lax.map(train_hop, (kernel, first, second, shifted_acts, shifted_grads))
        returned_all.append(jnp.roll(returned, hop_index, axis=0).reshape(TOK_ALL, D))
    return (jnp.roll(kernel, HOPS, axis=0), jnp.roll(first, HOPS, axis=0), jnp.roll(second, HOPS, axis=0), jnp.stack(returned_all))
```

```python
import jax
import jax.numpy as jnp
from jax import lax
from jax.sharding import PartitionSpec as P

HOPS = 3


def passed_along(part, axis, by):
    devices = lax.axis_size(axis)
    return lax.ppermute(part, axis, [(i, (i + by) % devices) for i in range(devices)])


def gelu_slope(values):
    inner = 0.7978845608 * (values + 0.044715 * values * values * values)
    tanh_part = jnp.tanh(inner)
    return 0.5 * (1.0 + tanh_part) + 0.5 * values * (1.0 - tanh_part * tanh_part) * 0.7978845608 * (
        1.0 + 0.134145 * values * values
    )


def slopes_of(kernel, inputs, grad_out):
    preact = jnp.dot(inputs, kernel, preferred_element_type=jnp.float32)
    return (grad_out.astype(jnp.float32) * gelu_slope(preact)).astype(jnp.bfloat16)


def update(kernel, first, second, inputs, slopes):
    gradient = lax.dot_general(
        inputs, slopes, (((0,), (0,)), ((), ())), preferred_element_type=jnp.float32
    )
    first = 0.9 * first.astype(jnp.float32) + 0.1 * gradient
    second = 0.95 * second.astype(jnp.float32) + 0.05 * gradient * gradient
    kernel = (kernel.astype(jnp.float32) - 0.01 * first / (jnp.sqrt(second) + 1e-08)).astype(
        jnp.bfloat16
    )
    return kernel, first, second


def returned_sum(slopes, kernel):
    shards = lax.axis_size("shard")
    me = lax.axis_index("shard")
    rows = slopes.shape[0] // shards

    def part(owner):
        mine = lax.dynamic_slice_in_dim(slopes, owner * rows, rows, 0)
        return lax.dot_general(
            mine, kernel, (((1,), (1,)), ((), ())), preferred_element_type=jnp.float32
        )

    arrived = [
        passed_along(part((me + k) % shards).astype(jnp.bfloat16), "shard", k)
        for k in range(1, shards)
    ]
    total = part(me)
    for piece in arrived:
        total = total + piece.astype(jnp.float32)
    return total.astype(jnp.bfloat16)


def shards(cut_acts, upstream, weights, moment_one, moment_two):
    kernel, first, second = weights[0], moment_one[0], moment_two[0]
    after = passed_along((cut_acts, upstream), "blk", -1)
    before = passed_along((cut_acts, upstream), "blk", 1)

    slopes = slopes_of(kernel, cut_acts, upstream)
    returned = [returned_sum(slopes, kernel)]
    kernel, first, second = update(kernel, first, second, cut_acts, slopes)

    slopes = slopes_of(kernel, *after)
    back = returned_sum(slopes, kernel)
    kernel, first, second = update(kernel, first, second, after[0], slopes)
    kernel = passed_along(kernel, "blk", HOPS)
    first = passed_along(first.astype(jnp.bfloat16), "blk", HOPS)
    second = passed_along(second.astype(jnp.bfloat16), "blk", HOPS)
    returned.append(passed_along(back, "blk", 1))

    slopes = slopes_of(kernel, *before)
    returned.append(passed_along(returned_sum(slopes, kernel), "blk", -1))
    kernel, first, second = update(kernel, first, second, before[0], slopes)
    return (kernel[None], first[None], second[None], jnp.stack(returned))


def solution(mesh):
    placed = (
        P("blk", None),
        P("blk", "shard"),
        P("blk", None, "shard"),
        P("blk", None, "shard"),
        P("blk", None, "shard"),
    )
    return jax.shard_map(
        shards,
        mesh=mesh,
        in_specs=placed,
        out_specs=(
            P("blk", None, "shard"),
            P("blk", None, "shard"),
            P("blk", None, "shard"),
            P(None, ("blk", "shard"), None),
        ),
        check_vma=False,
    )
```

```python
import functools

import jax
import jax.numpy as jnp
from jax import lax
from jax.experimental import pallas as pl
from jax.experimental.pallas import tpu as pltpu
from jax.sharding import PartitionSpec as P


HOPS = 3
F32, BF16 = jnp.float32, jnp.bfloat16
ANY = pl.BlockSpec(memory_space=pl.ANY)
WHOLE = pl.BlockSpec(memory_space=pltpu.VMEM)
MIB = 1024 * 1024


def passed_along(part, axis, by):
    devices = lax.axis_size(axis)
    return lax.ppermute(part, axis, [(i, (i + by) % devices) for i in range(devices)])


def routed(part, route):
    return jax.tree.map(lambda one: lax.ppermute(one, "blk", sorted(route.items())), part)


def only_if(chosen, body):
    if chosen is None:
        body()
    else:
        pl.when(chosen)(body)


def gelu_slope(values):
    square = values * values
    tanh_part = jnp.tanh(values * (0.7978845608 + 0.7978845608 * 0.044715 * square))
    return (0.5 + 0.5 * tanh_part) + (values * (1.0 - tanh_part * tanh_part)) * (
        0.5 * 0.7978845608 + 0.5 * 0.7978845608 * 0.134145 * square
    )


def blocks(size, step):
    step = step if size % step == 0 else size
    return [pl.ds(at, step) for at in range(0, size, step)]


def slopes_body(x, g, w, z, s):
    for cols in blocks(g.shape[1], 256):
        z[:, cols] = jnp.dot(x[...], w[:, cols], preferred_element_type=F32)
        for rows in blocks(x.shape[0], 64):
            s[rows, cols] = (g[rows, cols].astype(F32) * gelu_slope(z[rows, cols])).astype(BF16)


def update_rows(grad, w, m, v, w_new, m_new, v_new, rows):
    for at in blocks(rows.size, 32):
        at = pl.ds(rows.start + at.start, at.size)
        gradient = grad[at, :]
        first = 0.9 * m[at, :].astype(F32) + 0.1 * gradient
        second = 0.95 * v[at, :].astype(F32) + 0.05 * (gradient * gradient)
        m_new[at, :] = first.astype(m_new.dtype)
        v_new[at, :] = second.astype(v_new.dtype)
        root = second * lax.rsqrt(second)
        inverse = lax.rsqrt(second + 1e-08 * (2.0 * root + 1e-08))
        w_new[at, :] = (w[at, :].astype(F32) - (0.01 * first) * inverse).astype(BF16)


def train_kernel(parity, refs):
    if parity is None:
        train_body(*refs)
    else:
        pl.when(lax.rem(lax.axis_index("blk"), 2) == parity)(lambda: train_body(*refs))


def train_body(x_in, g_in, w_in, moments, w_out, mv_out, s_out, h_out,
               x, xt, g, w, m, v, z, s, grad, w_new, m_new, v_new, sem):
    m_in, v_in = (moments[0].at[0], moments[0].at[1]) if len(moments) == 1 else moments
    bands = blocks(w.shape[0], 256)
    n = len(bands)
    gets = [pltpu.make_async_copy(one, ref, sem.at[i]) for i, (one, ref) in enumerate(((x_in, x), (w_in, w), (g_in, g)))]
    gets += [
        pltpu.make_async_copy(one.at[band], ref.at[band], sem.at[3 + 2 * i + k])
        for i, band in enumerate(bands)
        for k, (one, ref) in enumerate(((m_in, m), (v_in, v)))
    ]
    for get in gets:
        get.start()
    for get in gets[:3]:
        get.wait()
    puts = []
    if h_out is not None:
        share = h_out.shape[1]
        at = pl.multiple_of(lax.axis_index("shard") * share, share)
        puts.append(pltpu.make_async_copy(x.at[:, pl.ds(at, share)], h_out, sem.at[0]))
        puts[0].start()
    xt[...] = x[...].T
    slopes_body(x, g, w, z, s)
    puts.append(pltpu.make_async_copy(s, s_out, sem.at[1]))
    puts[-1].start()
    for i, band in enumerate(bands):
        grad[band, :] = jnp.dot(xt[band, :], s[...], preferred_element_type=F32)
        for get in gets[3 + 2 * i : 5 + 2 * i]:
            get.wait()
        update_rows(grad, w, m, v, w_new, m_new, v_new, band)
        at = 3 + 2 * n + 3 * i
        new = [
            pltpu.make_async_copy(w_new.at[band], w_out.at[band], sem.at[at]),
            pltpu.make_async_copy(m_new.at[band], mv_out.at[0, band], sem.at[at + 1]),
            pltpu.make_async_copy(v_new.at[band], mv_out.at[1, band], sem.at[at + 2]),
        ]
        for put in new:
            put.start()
        puts += new
    for put in puts:
        put.wait()


def train(inputs, grad_out, kernel, moments, out_dtype, parity=None, share=None):
    tokens, depth = inputs.shape
    width = grad_out.shape[1]
    n = len(blocks(depth, 256))
    outs = [
        jax.ShapeDtypeStruct((depth, width), BF16),
        jax.ShapeDtypeStruct((2, depth, width), out_dtype),
        jax.ShapeDtypeStruct((tokens, width), BF16),
    ]
    if share is not None:
        outs.append(jax.ShapeDtypeStruct((tokens, share), BF16))

    def body(*refs):
        x_in, g_in, w_in, *refs = refs
        given, refs = refs[: len(moments)], refs[len(moments) :]
        out, scratch = list(refs[: len(outs)]), refs[len(outs) :]
        out += [None] * (4 - len(out))
        train_kernel(parity, (x_in, g_in, w_in, given, *out, *scratch))

    return pl.pallas_call(
        body,
        out_shape=tuple(outs),
        in_specs=[ANY] * (3 + len(moments)),
        out_specs=(ANY,) * len(outs),
        scratch_shapes=[
            pltpu.VMEM((tokens, depth), BF16),
            pltpu.VMEM((depth, tokens), BF16),
            pltpu.VMEM((tokens, width), BF16),
            pltpu.VMEM((depth, width), BF16),
            pltpu.VMEM((depth, width), F32),
            pltpu.VMEM((depth, width), F32),
            pltpu.VMEM((tokens, width), F32),
            pltpu.VMEM((tokens, width), BF16),
            pltpu.VMEM((depth, width), F32),
            pltpu.VMEM((depth, width), BF16),
            pltpu.VMEM((depth, width), out_dtype),
            pltpu.VMEM((depth, width), out_dtype),
            pltpu.SemaphoreType.DMA((3 + 5 * n,)),
        ],
        compiler_params=pltpu.CompilerParams(vmem_limit_bytes=60 * MIB),
        cost_estimate=pl.CostEstimate(
            flops=4 * tokens * depth * width, bytes_accessed=16 * depth * width, transcendentals=0
        ),
    )(inputs, grad_out, kernel, *moments)


def part_kernel(shift, n, several, *refs):
    slopes, (w_in, *arrived, out) = refs[:several], refs[several:]
    owner = lax.rem(lax.axis_index("shard") + shift, n)
    rows = slopes[0].shape[0] // n
    at = pl.ds(pl.multiple_of(owner * rows, rows), rows)
    for parity, s_in in enumerate(slopes):

        def body(s_in=s_in):
            total = lax.dot_general(s_in[at, :], w_in[...], (((1,), (1,)), ((), ())), preferred_element_type=F32)
            for piece in arrived:
                total = total + piece[...].astype(F32)
            out[...] = total.astype(BF16)

        only_if(None if several == 1 else lax.rem(lax.axis_index("blk"), 2) == parity, body)


def part(slopes, kernel, shift, arrived=()):
    n = lax.axis_size("shard")
    rows, depth = slopes[0].shape[0] // n, kernel.shape[0]
    return pl.pallas_call(
        functools.partial(part_kernel, shift, n, len(slopes)),
        out_shape=jax.ShapeDtypeStruct((rows, depth), BF16),
        compiler_params=pltpu.CompilerParams(vmem_limit_bytes=16 * MIB),
        cost_estimate=pl.CostEstimate(flops=2 * rows * kernel.size, bytes_accessed=2 * kernel.size, transcendentals=0),
        name="part",
    )(*slopes, kernel, *arrived)


def from_one_of(chosen, dst, sem):
    for condition, src in chosen:
        pl.when(condition)(lambda src=src: pltpu.make_async_copy(src, dst, sem).start())
    return pltpu.make_async_copy(chosen[0][1], dst, sem)


def sources():
    n = lax.axis_size("blk")
    return lax.rem(lax.axis_index("blk") + (n - HOPS % n), n)


def forward_kernel(shards, *refs):
    halves, (g_in, w_even, w_odd, s, w, xt, x, g, z, sem) = refs[:shards], refs[shards:]
    me = lax.axis_index("shard")
    share = halves[0].shape[1]
    gets = []
    for k, half in enumerate(halves):
        owner = lax.rem(me + (shards - k), shards)
        at = pl.ds(pl.multiple_of(owner * share, share), share)
        gets.append(pltpu.make_async_copy(half, x.at[:, at], sem.at[k]))
    gets.append(pltpu.make_async_copy(g_in, g, sem.at[shards]))
    for get in gets:
        get.start()
    odd = lax.rem(sources(), 2)
    gets.append(from_one_of([(odd == 0, w_even), (odd == 1, w_odd)], w, sem.at[shards + 1]))
    for get in gets:
        get.wait()
    slopes_body(x, g, w, z, s)
    xt[...] = x[...].T


def forward(halves, grad_out, even, odd):
    tokens, width = grad_out.shape
    depth = even.shape[0]
    n = len(halves)
    return pl.pallas_call(
        functools.partial(forward_kernel, n),
        out_shape=(
            jax.ShapeDtypeStruct((tokens, width), BF16),
            jax.ShapeDtypeStruct((depth, width), BF16),
            jax.ShapeDtypeStruct((depth, tokens), BF16),
        ),
        in_specs=[ANY] * (n + 3),
        out_specs=(WHOLE,) * 3,
        scratch_shapes=[
            pltpu.VMEM((tokens, depth), BF16),
            pltpu.VMEM((tokens, width), BF16),
            pltpu.VMEM((tokens, width), F32),
            pltpu.SemaphoreType.DMA((n + 2,)),
        ],
        compiler_params=pltpu.CompilerParams(vmem_limit_bytes=16 * MIB),
        cost_estimate=pl.CostEstimate(
            flops=2 * tokens * depth * width, bytes_accessed=4 * depth * width, transcendentals=0
        ),
        name="forward",
    )(*halves, grad_out, even, odd)


def gradient_kernel(xt, s, grad):
    grad[...] = jnp.dot(xt[...], s[...], preferred_element_type=F32)


def gradient(transposed, slopes):
    depth, tokens = transposed.shape
    width = slopes.shape[1]
    return pl.pallas_call(
        gradient_kernel,
        out_shape=jax.ShapeDtypeStruct((depth, width), F32),
        compiler_params=pltpu.CompilerParams(vmem_limit_bytes=16 * MIB),
        cost_estimate=pl.CostEstimate(
            flops=2 * tokens * depth * width, bytes_accessed=4 * depth * width, transcendentals=0
        ),
        name="gradient",
    )(transposed, slopes)


def finish_kernel(detour, grad, w, mv_even, mv_odd, *rest):
    mv_detour, rest = (rest[0], rest[1:]) if detour else (None, rest)
    *returned, w_out, m_out, v_out, r_out, m, v, w_new, m_new, v_new, sem = rest
    bands = blocks(w.shape[0], 256)
    origin = sources()
    chosen = [(lax.rem(origin, 2) == 1, mv_odd)]
    if detour:
        chosen += [(lax.rem(origin, 4) == 0, mv_even), (lax.rem(origin, 4) == 2, mv_detour)]
    else:
        chosen += [(lax.rem(origin, 2) == 0, mv_even)]
    gets = [
        [
            from_one_of([(when, mv.at[k, band]) for when, mv in chosen], ref.at[band], sem.at[5 * i + k])
            for k, ref in enumerate((m, v))
        ]
        for i, band in enumerate(bands)
    ]
    puts = [
        pltpu.make_async_copy(one, r_out.at[i], sem.at[5 * len(bands) + i]) for i, one in enumerate(returned)
    ]
    for put in puts:
        put.start()
    for i, band in enumerate(bands):
        for get in gets[i]:
            get.wait()
        update_rows(grad, w, m, v, w_new, m_new, v_new, band)
        new = [
            pltpu.make_async_copy(one.at[band], out.at[band], sem.at[5 * i + 2 + k])
            for k, (one, out) in enumerate(((w_new, w_out), (m_new, m_out), (v_new, v_out)))
        ]
        for put in new:
            put.start()
        puts += new
    for put in puts:
        put.wait()


def finish(grad, kernel, moments, returned):
    depth, width = kernel.shape
    rows = returned[0].shape
    n = len(blocks(depth, 256))
    return pl.pallas_call(
        functools.partial(finish_kernel, len(moments) == 3),
        out_shape=(
            jax.ShapeDtypeStruct((depth, width), BF16),
            jax.ShapeDtypeStruct((depth, width), F32),
            jax.ShapeDtypeStruct((depth, width), F32),
            jax.ShapeDtypeStruct((len(returned),) + rows, BF16),
        ),
        in_specs=[WHOLE] * 2 + [ANY] * len(moments) + [WHOLE] * len(returned),
        out_specs=(ANY,) * 4,
        scratch_shapes=[
            pltpu.VMEM((depth, width), BF16),
            pltpu.VMEM((depth, width), BF16),
            pltpu.VMEM((depth, width), BF16),
            pltpu.VMEM((depth, width), F32),
            pltpu.VMEM((depth, width), F32),
            pltpu.SemaphoreType.DMA((5 * n + len(returned),)),
        ],
        compiler_params=pltpu.CompilerParams(vmem_limit_bytes=24 * MIB),
        cost_estimate=pl.CostEstimate(flops=30 * depth * width, bytes_accessed=16 * depth * width, transcendentals=0),
        name="finish",
    )(grad, kernel, *moments, *returned)


def shards(cut_acts, upstream, weights, moment_one, moment_two):
    kernel, first, second = weights[0], moment_one[0], moment_two[0]
    n, m = lax.axis_size("blk"), lax.axis_size("shard")
    evens, odds = range(0, n, 2), range(1, n, 2)
    to_far, to_near = {(i + 1) % n: i for i in odds}, {(i + 1) % n: i for i in evens}
    far = routed(cut_acts, to_far), routed(upstream, to_far)
    near = routed(cut_acts, to_near), routed(upstream, to_near)

    share = cut_acts.shape[1] // m
    kernel1, moments1, slopes0, half = train(cut_acts, upstream, kernel, (first, second), F32, share=share)
    half = passed_along(half, "blk", 1)
    grad_before = passed_along(upstream, "blk", 1)

    even_w, even_mv, slopes_even = train(*near, kernel1, (moments1,), BF16, parity=0)
    even_w = routed(even_w, {i: (i + HOPS) % n for i in evens})
    detour = n % 4 == 0
    even_mv = routed(even_mv, {i: i - 1 if detour and i % 4 == 2 else (i + HOPS) % n for i in evens})

    odd_w, odd_mv, slopes_odd = train(*far, kernel1, (moments1,), BF16, parity=1)
    odd_w = routed(odd_w, {i: (i + HOPS) % n for i in odds})
    odd_mv = routed(odd_mv, {i: (i + HOPS) % n for i in odds})

    def summed(slopes, kernel):
        parts = [part(slopes, kernel, k) for k in range(1, m)]
        parts = [passed_along(one, "shard", k + 1) for k, one in enumerate(parts)]
        return part(slopes, kernel, 0, parts)

    home = summed([slopes0], kernel)
    back = summed([slopes_even, slopes_odd], kernel1)
    back = passed_along(back, "blk", 1)

    halves = [half] + [passed_along(half, "shard", k) for k in range(1, m)]
    slopes2, moved, transposed = forward(halves, grad_before, even_w, odd_w)
    last = summed([slopes2], moved)
    last = passed_along(last, "blk", -1)
    grad2 = gradient(transposed, slopes2)
    moments = (even_mv, odd_mv)
    if detour:
        moments += (routed(even_mv, {i: (i + 1 + HOPS) % n for i in range(1, n, 4)}),)
    kernel3, first3, second3, returned = finish(grad2, moved, moments, (home, back, last))
    return (kernel3[None], first3[None], second3[None], returned)


def solution(mesh):
    placed = (
        P("blk", None),
        P("blk", "shard"),
        P("blk", None, "shard"),
        P("blk", None, "shard"),
        P("blk", None, "shard"),
    )
    return jax.shard_map(
        shards,
        mesh=mesh,
        in_specs=placed,
        out_specs=(
            P("blk", None, "shard"),
            P("blk", None, "shard"),
            P("blk", None, "shard"),
            P(None, ("blk", "shard"), None),
        ),
        check_vma=False,
    )
```

```python
import functools

import jax
import jax.numpy as jnp
from jax import lax
from jax.experimental import pallas as pl
from jax.experimental.pallas import tpu as pltpu
from jax.sharding import PartitionSpec as P


HOPS = 3
F32, BF16 = jnp.float32, jnp.bfloat16
ANY = pl.BlockSpec(memory_space=pl.ANY)
WHOLE = pl.BlockSpec(memory_space=pltpu.VMEM)
MIB = 1024 * 1024


def passed_along(part, axis, by):
    devices = lax.axis_size(axis)
    return lax.ppermute(part, axis, [(i, (i + by) % devices) for i in range(devices)])


def routed(part, route):
    return jax.tree.map(lambda one: lax.ppermute(one, "blk", sorted(route.items())), part)


def only_if(chosen, body):
    if chosen is None:
        body()
    else:
        pl.when(chosen)(body)


def gelu_slope(values):
    square = values * values
    tanh_part = jnp.tanh(values * (0.7978845608 + 0.7978845608 * 0.044715 * square))
    return (0.5 + 0.5 * tanh_part) + (values * (1.0 - tanh_part * tanh_part)) * (
        0.5 * 0.7978845608 + 0.5 * 0.7978845608 * 0.134145 * square
    )


def blocks(size, step):
    step = step if size % step == 0 else size
    return [pl.ds(at, step) for at in range(0, size, step)]


def slopes_body(x, g, w, z, s):
    for cols in blocks(g.shape[1], 256):
        z[:, cols] = jnp.dot(x[...], w[:, cols], preferred_element_type=F32)
        for rows in blocks(x.shape[0], 64):
            s[rows, cols] = (g[rows, cols].astype(F32) * gelu_slope(z[rows, cols])).astype(BF16)


def update_rows(grad, w, m, v, w_new, m_new, v_new, rows):
    for at in blocks(rows.size, 32):
        at = pl.ds(rows.start + at.start, at.size)
        gradient = grad[at, :]
        first = 0.9 * m[at, :].astype(F32) + 0.1 * gradient
        second = 0.95 * v[at, :].astype(F32) + 0.05 * (gradient * gradient)
        m_new[at, :] = first.astype(m_new.dtype)
        v_new[at, :] = second.astype(v_new.dtype)
        root = second * lax.rsqrt(second)
        inverse = lax.rsqrt(second + 1e-08 * (2.0 * root + 1e-08))
        w_new[at, :] = (w[at, :].astype(F32) - (0.01 * first) * inverse).astype(BF16)


def copies_of(parts, whole, sems):
    if len(parts) == 1:
        return [pltpu.make_async_copy(parts[0], whole, sems[0])]
    shards = len(parts)
    me = lax.axis_index("shard")
    share = parts[0].shape[1]
    copies = []
    for k, one in enumerate(parts):
        owner = lax.rem(me + (shards - k), shards)
        at = pl.ds(pl.multiple_of(owner * share, share), share)
        copies.append(pltpu.make_async_copy(one, whole.at[:, at], sems[k]))
    return copies


def train_body(x_in, g_in, w_in, m_in, v_in, w_out, m_out, v_out, s_out,
               x, xt, g, w, m, v, z, s, grad, w_new, m_new, v_new, sem):
    bands = blocks(w.shape[0], 256)
    n = len(bands)
    last = 3 + 5 * n
    get_x = copies_of(x_in, x, [sem.at[last + k] for k in range(len(x_in))])
    get_w, get_g = [
        pltpu.make_async_copy(one, ref, sem.at[1 + i]) for i, (one, ref) in enumerate(((w_in, w), (g_in, g)))
    ]
    gets = [
        [
            pltpu.make_async_copy(one.at[band], ref.at[band], sem.at[3 + 2 * i + k])
            for k, (one, ref) in enumerate(((m_in, m), (v_in, v)))
        ]
        for i, band in enumerate(bands)
    ]
    for get in get_x + [get_w, get_g]:
        get.start()
    for get in get_x:
        get.wait()
    for get in gets[0]:
        get.start()
    puts = []
    xt[...] = x[...].T
    get_w.wait()
    get_g.wait()
    for pair in gets[1:]:
        for get in pair:
            get.start()
    slopes_body(x, g, w, z, s)
    puts.append(pltpu.make_async_copy(s, s_out, sem.at[0]))
    puts[-1].start()
    for i, band in enumerate(bands):
        grad[band, :] = jnp.dot(xt[band, :], s[...], preferred_element_type=F32)
        for get in gets[i]:
            get.wait()
        update_rows(grad, w, m, v, w_new, m_new, v_new, band)
        new = [
            pltpu.make_async_copy(one.at[band], out.at[band], sem.at[3 + 2 * n + 3 * i + k])
            for k, (one, out) in enumerate(((w_new, w_out), (m_new, m_out), (v_new, v_out)))
        ]
        for put in new:
            put.start()
        puts += new
    for put in puts:
        put.wait()


def train(inputs, grad_out, kernel, first, second, out_dtype, parity=None):
    (tokens, width), depth = grad_out.shape, kernel.shape[0]
    k = len(inputs)
    n = len(blocks(depth, 256))
    outs = [
        jax.ShapeDtypeStruct((depth, width), BF16),
        jax.ShapeDtypeStruct((depth, width), out_dtype),
        jax.ShapeDtypeStruct((depth, width), out_dtype),
        jax.ShapeDtypeStruct((tokens, width), BF16),
    ]

    def body(*refs):
        only_if(
            None if parity is None else lax.rem(lax.axis_index("blk"), 2) == parity,
            lambda: train_body(refs[:k], *refs[k:]),
        )

    return pl.pallas_call(
        body,
        out_shape=tuple(outs),
        in_specs=[ANY] * (k + 4),
        out_specs=(ANY,) * len(outs),
        scratch_shapes=[
            pltpu.VMEM((tokens, depth), BF16),
            pltpu.VMEM((depth, tokens), BF16),
            pltpu.VMEM((tokens, width), BF16),
            pltpu.VMEM((depth, width), BF16),
            pltpu.VMEM((depth, width), F32),
            pltpu.VMEM((depth, width), F32),
            pltpu.VMEM((tokens, width), F32),
            pltpu.VMEM((tokens, width), BF16),
            pltpu.VMEM((depth, width), F32),
            pltpu.VMEM((depth, width), BF16),
            pltpu.VMEM((depth, width), out_dtype),
            pltpu.VMEM((depth, width), out_dtype),
            pltpu.SemaphoreType.DMA((3 + 5 * n + k,)),
        ],
        compiler_params=pltpu.CompilerParams(vmem_limit_bytes=(60 if parity is None else 48) * MIB),
        cost_estimate=pl.CostEstimate(
            flops=4 * tokens * depth * width, bytes_accessed=16 * depth * width, transcendentals=0
        ),
    )(*inputs, grad_out, kernel, first, second)


def part_kernel(shift, n, several, *refs):
    slopes, (w_in, *arrived, out) = refs[:several], refs[several:]
    owner = lax.rem(lax.axis_index("shard") + shift, n)
    rows = slopes[0].shape[0] // n
    at = pl.ds(pl.multiple_of(owner * rows, rows), rows)
    for parity, s_in in enumerate(slopes):

        def body(s_in=s_in):
            total = lax.dot_general(s_in[at, :], w_in[...], (((1,), (1,)), ((), ())), preferred_element_type=F32)
            for piece in arrived:
                total = total + piece[...].astype(F32)
            out[...] = total.astype(BF16)

        only_if(None if several == 1 else lax.rem(lax.axis_index("blk"), 2) == parity, body)


def part(slopes, kernel, shift, arrived=()):
    n = lax.axis_size("shard")
    rows, depth = slopes[0].shape[0] // n, kernel.shape[0]
    return pl.pallas_call(
        functools.partial(part_kernel, shift, n, len(slopes)),
        out_shape=jax.ShapeDtypeStruct((rows, depth), BF16),
        compiler_params=pltpu.CompilerParams(vmem_limit_bytes=16 * MIB),
        cost_estimate=pl.CostEstimate(flops=2 * rows * kernel.size, bytes_accessed=2 * kernel.size, transcendentals=0),
        name="part",
    )(*slopes, kernel, *arrived)


def from_one_of(chosen, dst, sem):
    for condition, src in chosen:
        pl.when(condition)(lambda src=src: pltpu.make_async_copy(src, dst, sem).start())
    return pltpu.make_async_copy(chosen[0][1], dst, sem)


def sources():
    n = lax.axis_size("blk")
    return lax.rem(lax.axis_index("blk") + (n - HOPS % n), n)


def forward_kernel(shards, *refs):
    across, (x_near, g_across, g_near, w_even, w_odd, s, w, xt, x, g, z, sem) = refs[:shards], refs[shards:]
    odd_here = lax.rem(lax.axis_index("blk"), 2) == 1
    odd_source = lax.rem(sources(), 2) == 1

    def start(copies):
        for copy in copies:
            copy.start()

    def wait(copies):
        for copy in copies:
            copy.wait()

    sems = [sem.at[k] for k in range(shards)]
    pl.when(odd_here)(lambda: start(copies_of([x_near], x, sems)))
    pl.when(jnp.logical_not(odd_here))(lambda: start(copies_of(across, x, sems)))
    gets = [
        from_one_of([(jnp.logical_not(odd_here), g_across), (odd_here, g_near)], g, sem.at[shards]),
        from_one_of([(jnp.logical_not(odd_source), w_even), (odd_source, w_odd)], w, sem.at[shards + 1]),
    ]
    pl.when(odd_here)(lambda: wait(copies_of([x_near], x, sems)))
    pl.when(jnp.logical_not(odd_here))(lambda: wait(copies_of(across, x, sems)))
    wait(gets)
    slopes_body(x, g, w, z, s)
    xt[...] = x[...].T


def forward(across, x_near, g_across, g_near, even, odd):
    (tokens, width), depth = g_near.shape, even.shape[0]
    n = len(across)
    return pl.pallas_call(
        functools.partial(forward_kernel, n),
        out_shape=(
            jax.ShapeDtypeStruct((tokens, width), BF16),
            jax.ShapeDtypeStruct((depth, width), BF16),
            jax.ShapeDtypeStruct((depth, tokens), BF16),
        ),
        in_specs=[ANY] * (n + 5),
        out_specs=(WHOLE,) * 3,
        scratch_shapes=[
            pltpu.VMEM((tokens, depth), BF16),
            pltpu.VMEM((tokens, width), BF16),
            pltpu.VMEM((tokens, width), F32),
            pltpu.SemaphoreType.DMA((n + 2,)),
        ],
        compiler_params=pltpu.CompilerParams(vmem_limit_bytes=16 * MIB),
        cost_estimate=pl.CostEstimate(
            flops=2 * tokens * depth * width, bytes_accessed=4 * depth * width, transcendentals=0
        ),
        name="forward",
    )(*across, x_near, g_across, g_near, even, odd)


def gradient_kernel(xt, s, grad):
    grad[...] = jnp.dot(xt[...], s[...], preferred_element_type=F32)


def gradient(transposed, slopes):
    depth, tokens = transposed.shape
    width = slopes.shape[1]
    return pl.pallas_call(
        gradient_kernel,
        out_shape=jax.ShapeDtypeStruct((depth, width), F32),
        compiler_params=pltpu.CompilerParams(vmem_limit_bytes=16 * MIB),
        cost_estimate=pl.CostEstimate(
            flops=2 * tokens * depth * width, bytes_accessed=4 * depth * width, transcendentals=0
        ),
        name="gradient",
    )(transposed, slopes)


def finish_kernel(shards, moments, grad, w, *refs):
    given, refs = refs[:moments], refs[moments:]
    home, back, refs = refs[0], refs[1], refs[2:]
    last, (w_out, m_out, v_out, r_out, m, v, w_new, m_new, v_new, r, sem) = refs[:shards], refs[shards:]
    m_even, v_even, m_odd, v_odd, *m_detour = given
    bands = blocks(w.shape[0], 256)
    n = len(bands)
    origin = sources()
    even, odd = lax.rem(origin, 2) == 0, lax.rem(origin, 2) == 1
    m_from, v_from = [(odd, m_odd)], [(even, v_even), (odd, v_odd)]
    if m_detour:
        m_from += [(lax.rem(origin, 4) == 0, m_even), (lax.rem(origin, 4) == 2, m_detour[0])]
    else:
        m_from += [(even, m_even)]
    gets = [
        [
            from_one_of([(when, one.at[band]) for when, one in chosen], ref.at[band], sem.at[5 * i + k])
            for k, (chosen, ref) in enumerate(((m_from, m), (v_from, v)))
        ]
        for i, band in enumerate(bands)
    ]
    total = last[0][...].astype(F32)
    for piece in last[1:]:
        total = total + piece[...].astype(F32)
    r[...] = total.astype(BF16)
    puts = [
        pltpu.make_async_copy(one, r_out.at[i], sem.at[5 * n + i]) for i, one in enumerate((home, back, r))
    ]
    for put in puts:
        put.start()
    for i, band in enumerate(bands):
        for get in gets[i]:
            get.wait()
        update_rows(grad, w, m, v, w_new, m_new, v_new, band)
        new = [
            pltpu.make_async_copy(one.at[band], out.at[band], sem.at[5 * i + 2 + k])
            for k, (one, out) in enumerate(((w_new, w_out), (m_new, m_out), (v_new, v_out)))
        ]
        for put in new:
            put.start()
        puts += new
    for put in puts:
        put.wait()


def finish(grad, kernel, moments, home, back, last):
    depth, width = kernel.shape
    rows = home.shape
    n = len(blocks(depth, 256))
    return pl.pallas_call(
        functools.partial(finish_kernel, len(last), len(moments)),
        out_shape=(
            jax.ShapeDtypeStruct((depth, width), BF16),
            jax.ShapeDtypeStruct((depth, width), F32),
            jax.ShapeDtypeStruct((depth, width), F32),
            jax.ShapeDtypeStruct((HOPS,) + rows, BF16),
        ),
        in_specs=[WHOLE] * 2 + [ANY] * len(moments) + [WHOLE] * (2 + len(last)),
        out_specs=(ANY,) * 4,
        scratch_shapes=[
            pltpu.VMEM((depth, width), BF16),
            pltpu.VMEM((depth, width), BF16),
            pltpu.VMEM((depth, width), BF16),
            pltpu.VMEM((depth, width), F32),
            pltpu.VMEM((depth, width), F32),
            pltpu.VMEM(rows, BF16),
            pltpu.SemaphoreType.DMA((5 * n + HOPS,)),
        ],
        compiler_params=pltpu.CompilerParams(vmem_limit_bytes=24 * MIB),
        cost_estimate=pl.CostEstimate(flops=30 * depth * width, bytes_accessed=16 * depth * width, transcendentals=0),
        name="finish",
    )(grad, kernel, *moments, home, back, *last)


def shards(cut_acts, upstream, weights, moment_one, moment_two):
    kernel, first, second = weights[0], moment_one[0], moment_two[0]
    n, m = lax.axis_size("blk"), lax.axis_size("shard")
    evens, odds = range(0, n, 2), range(1, n, 2)
    share = cut_acts.shape[1] // m
    half = lax.dynamic_slice_in_dim(cut_acts, lax.axis_index("shard") * share, share, 1)
    pairs = n - n % 2
    partner = {i: i ^ 1 if i < pairs else i for i in range(n)}
    neighbour = {i: (i + 1) % n if i % 2 else (i - 1) % n for i in range(n)}
    across = [routed(half, neighbour)]
    across_g = passed_along(upstream, "blk", -1)
    near_x, near_g = routed(cut_acts, partner), routed(upstream, partner)
    kernel1, first1, second1, slopes0 = train([cut_acts], upstream, kernel, first, second, F32)
    across += [passed_along(across[0], "shard", k) for k in range(1, m)]
    before_g = passed_along(upstream, "blk", 1)

    detour = n % 4 == 0
    even_to, odd_to = {i: (i + HOPS) % n for i in evens}, {i: (i + HOPS) % n for i in odds}
    first_to = {i: i - 1 if detour and i % 4 == 2 else to for i, to in even_to.items()}
    odd_to |= {i: partner[i] for i in evens}
    even_to |= {i: partner[i] for i in odds}
    first_to |= {i: partner[i] for i in odds}
    even_w, even_m, even_v, slopes_even = train([near_x], near_g, kernel1, first1, second1, BF16, parity=0)
    even_w = routed(even_w, even_to)
    even_m = routed(even_m, first_to)
    even_v = routed(even_v, even_to)
    odd_w, odd_m, odd_v, slopes_odd = train(across, across_g, kernel1, first1, second1, BF16, parity=1)
    odd_w = routed(odd_w, odd_to)
    odd_m = routed(odd_m, odd_to)
    odd_v = routed(odd_v, odd_to)
    moments = (even_m, even_v, odd_m, odd_v)
    if detour:
        moments += (routed(even_m, {i: (i + 1 + HOPS) % n for i in range(1, n, 4)}),)

    def summed(slopes, kernel):
        parts = [part(slopes, kernel, k) for k in range(1, m)]
        parts = [passed_along(one, "shard", k + 1) for k, one in enumerate(parts)]
        return part(slopes, kernel, 0, parts)

    home = summed([slopes0], kernel)
    back = summed([slopes_even, slopes_odd], kernel1)
    back = passed_along(back, "blk", 1)

    slopes2, moved, transposed = forward(across, near_x, before_g, near_g, even_w, odd_w)
    last = passed_along(summed([slopes2], moved), "blk", -1)
    grad2 = gradient(transposed, slopes2)
    kernel3, first3, second3, returned = finish(grad2, moved, moments, home, back, [last])
    return (kernel3[None], first3[None], second3[None], returned)


def solution(mesh):
    placed = (
        P("blk", None),
        P("blk", "shard"),
        P("blk", None, "shard"),
        P("blk", None, "shard"),
        P("blk", None, "shard"),
    )
    return jax.shard_map(
        shards,
        mesh=mesh,
        in_specs=placed,
        out_specs=(
            P("blk", None, "shard"),
            P("blk", None, "shard"),
            P("blk", None, "shard"),
            P(None, ("blk", "shard"), None),
        ),
        check_vma=False,
    )
```

```python
import functools

import jax
import jax.numpy as jnp
from jax import lax
from jax.experimental import pallas as pl
from jax.experimental.pallas import tpu as pltpu
from jax.sharding import PartitionSpec as P


HOPS = 3
F32, BF16 = jnp.float32, jnp.bfloat16
ANY = pl.BlockSpec(memory_space=pl.ANY)
WHOLE = pl.BlockSpec(memory_space=pltpu.VMEM)
MIB = 1024 * 1024
CUT_FLOPS = 4 * 10**9


def passed_along(part, axis, by):
    devices = lax.axis_size(axis)
    return lax.ppermute(part, axis, [(i, (i + by) % devices) for i in range(devices)])


def routed(part, route):
    return jax.tree.map(lambda one: lax.ppermute(one, "blk", sorted(route.items())), part)


def only_if(chosen, body):
    if chosen is None:
        body()
    else:
        pl.when(chosen)(body)


def gelu_slope(values):
    square = values * values
    tanh_part = jnp.tanh(values * (0.7978845608 + 0.7978845608 * 0.044715 * square))
    return (0.5 + 0.5 * tanh_part) + (values * (1.0 - tanh_part * tanh_part)) * (
        0.5 * 0.7978845608 + 0.5 * 0.7978845608 * 0.134145 * square
    )


def blocks(size, step):
    step = step if size % step == 0 else size
    return [pl.ds(at, step) for at in range(0, size, step)]


def slopes_body(x, g, w, z, s):
    for cols in blocks(g.shape[1], 256):
        z[:, cols] = jnp.dot(x[...], w[:, cols], preferred_element_type=F32)
        for rows in blocks(x.shape[0], 64):
            s[rows, cols] = (g[rows, cols].astype(F32) * gelu_slope(z[rows, cols])).astype(BF16)


def update_rows(grad, w, m, v, w_new, m_new, v_new, rows):
    for at in blocks(rows.size, 32):
        at = pl.ds(rows.start + at.start, at.size)
        gradient = grad[at, :]
        first = 0.9 * m[at, :].astype(F32) + 0.1 * gradient
        second = 0.95 * v[at, :].astype(F32) + 0.05 * (gradient * gradient)
        m_new[at, :] = first.astype(m_new.dtype)
        v_new[at, :] = second.astype(v_new.dtype)
        root = second * lax.rsqrt(second)
        inverse = lax.rsqrt(second + 1e-08 * (2.0 * root + 1e-08))
        w_new[at, :] = (w[at, :].astype(F32) - (0.01 * first) * inverse).astype(BF16)


def copies_of(parts, whole, sems):
    if len(parts) == 1:
        return [pltpu.make_async_copy(parts[0], whole, sems[0])]
    shards = len(parts)
    me = lax.axis_index("shard")
    share = parts[0].shape[1]
    copies = []
    for k, one in enumerate(parts):
        owner = lax.rem(me + (shards - k), shards)
        at = pl.ds(pl.multiple_of(owner * share, share), share)
        copies.append(pltpu.make_async_copy(one, whole.at[:, at], sems[k]))
    return copies


def train_body(fetched, x_in, g_in, w, m, v, w_new, m_new, v_new, s, xt, z, grad, *scratch):
    if fetched:
        x, g, sem = scratch
        gets = copies_of(x_in, x, [sem.at[1 + k] for k in range(len(x_in))])
        gets.append(pltpu.make_async_copy(g_in, g, sem.at[0]))
        for get in gets:
            get.start()
        for get in gets:
            get.wait()
    else:
        x, g = x_in[0], g_in
    xt[...] = x[...].T
    slopes_body(x, g, w, z, s)
    for band in blocks(w.shape[0], 256):
        grad[band, :] = jnp.dot(xt[band, :], s[...], preferred_element_type=F32)
        update_rows(grad, w, m, v, w_new, m_new, v_new, band)


def train(inputs, grad_out, kernel, first, second, out_dtype, parity=None):
    (tokens, width), depth = grad_out.shape, kernel.shape[0]
    k = len(inputs)

    def body(*refs):
        only_if(
            None if parity is None else lax.rem(lax.axis_index("blk"), 2) == parity,
            lambda: train_body(parity is not None, refs[:k], *refs[k:]),
        )

    scratch = [
        pltpu.VMEM((depth, tokens), BF16),
        pltpu.VMEM((tokens, width), F32),
        pltpu.VMEM((depth, width), F32),
    ]
    if parity is not None:
        scratch += [
            pltpu.VMEM((tokens, depth), BF16),
            pltpu.VMEM((tokens, width), BF16),
            pltpu.SemaphoreType.DMA((1 + k,)),
        ]
    return pl.pallas_call(
        body,
        out_shape=(
            jax.ShapeDtypeStruct((depth, width), BF16),
            jax.ShapeDtypeStruct((depth, width), out_dtype),
            jax.ShapeDtypeStruct((depth, width), out_dtype),
            jax.ShapeDtypeStruct((tokens, width), BF16),
        ),
        in_specs=[WHOLE if parity is None else ANY] * (k + 1) + [WHOLE] * 3,
        out_specs=(WHOLE,) * 4,
        scratch_shapes=scratch,
        compiler_params=pltpu.CompilerParams(vmem_limit_bytes=24 * MIB),
        cost_estimate=pl.CostEstimate(
            flops=4 * tokens * depth * width, bytes_accessed=16 * depth * width, transcendentals=0
        ),
    )(*inputs, grad_out, kernel, first, second)


def cut_kernel(x_in, out, sem):
    share = out.shape[1]
    at = pl.multiple_of(lax.axis_index("shard") * share, share)
    get = pltpu.make_async_copy(x_in.at[:, pl.ds(at, share)], out, sem)
    get.start()
    get.wait()


def cut(inputs, share):
    return pl.pallas_call(
        cut_kernel,
        out_shape=jax.ShapeDtypeStruct((inputs.shape[0], share), BF16),
        in_specs=[ANY],
        out_specs=WHOLE,
        scratch_shapes=[pltpu.SemaphoreType.DMA],
        compiler_params=pltpu.CompilerParams(vmem_limit_bytes=8 * MIB),
        cost_estimate=pl.CostEstimate(flops=CUT_FLOPS, bytes_accessed=4 * inputs.size, transcendentals=0),
        name="cut",
    )(inputs)


def part_kernel(shift, n, several, *refs):
    slopes, (w_in, *arrived, out) = refs[:several], refs[several:]
    owner = lax.rem(lax.axis_index("shard") + shift, n)
    rows = slopes[0].shape[0] // n
    at = pl.ds(pl.multiple_of(owner * rows, rows), rows)
    for parity, s_in in enumerate(slopes):

        def body(s_in=s_in):
            total = lax.dot_general(s_in[at, :], w_in[...], (((1,), (1,)), ((), ())), preferred_element_type=F32)
            for piece in arrived:
                total = total + piece[...].astype(F32)
            out[...] = total.astype(BF16)

        only_if(None if several == 1 else lax.rem(lax.axis_index("blk"), 2) == parity, body)


def part(slopes, kernel, shift, arrived=()):
    n = lax.axis_size("shard")
    rows, depth = slopes[0].shape[0] // n, kernel.shape[0]
    return pl.pallas_call(
        functools.partial(part_kernel, shift, n, len(slopes)),
        out_shape=jax.ShapeDtypeStruct((rows, depth), BF16),
        compiler_params=pltpu.CompilerParams(vmem_limit_bytes=16 * MIB),
        cost_estimate=pl.CostEstimate(flops=2 * rows * kernel.size, bytes_accessed=2 * kernel.size, transcendentals=0),
        name="part",
    )(*slopes, kernel, *arrived)


def from_one_of(chosen, dst, sem):
    for condition, src in chosen:
        pl.when(condition)(lambda src=src: pltpu.make_async_copy(src, dst, sem).start())
    return pltpu.make_async_copy(chosen[0][1], dst, sem)


def sources():
    n = lax.axis_size("blk")
    return lax.rem(lax.axis_index("blk") + (n - HOPS % n), n)


def forward_kernel(shards, *refs):
    across, (x_near, g_across, g_near, w_even, w_odd, s, w, xt, x, g, z, sem) = refs[:shards], refs[shards:]
    odd_here = lax.rem(lax.axis_index("blk"), 2) == 1
    odd_source = lax.rem(sources(), 2) == 1

    def start(copies):
        for copy in copies:
            copy.start()

    def wait(copies):
        for copy in copies:
            copy.wait()

    sems = [sem.at[k] for k in range(shards)]
    pl.when(odd_here)(lambda: start(copies_of([x_near], x, sems)))
    pl.when(jnp.logical_not(odd_here))(lambda: start(copies_of(across, x, sems)))
    gets = [
        from_one_of([(jnp.logical_not(odd_here), g_across), (odd_here, g_near)], g, sem.at[shards]),
        from_one_of([(jnp.logical_not(odd_source), w_even), (odd_source, w_odd)], w, sem.at[shards + 1]),
    ]
    pl.when(odd_here)(lambda: wait(copies_of([x_near], x, sems)))
    pl.when(jnp.logical_not(odd_here))(lambda: wait(copies_of(across, x, sems)))
    wait(gets)
    slopes_body(x, g, w, z, s)
    xt[...] = x[...].T


def forward(across, x_near, g_across, g_near, even, odd):
    (tokens, width), depth = g_near.shape, even.shape[0]
    n = len(across)
    return pl.pallas_call(
        functools.partial(forward_kernel, n),
        out_shape=(
            jax.ShapeDtypeStruct((tokens, width), BF16),
            jax.ShapeDtypeStruct((depth, width), BF16),
            jax.ShapeDtypeStruct((depth, tokens), BF16),
        ),
        in_specs=[ANY] * (n + 5),
        out_specs=(WHOLE,) * 3,
        scratch_shapes=[
            pltpu.VMEM((tokens, depth), BF16),
            pltpu.VMEM((tokens, width), BF16),
            pltpu.VMEM((tokens, width), F32),
            pltpu.SemaphoreType.DMA((n + 2,)),
        ],
        compiler_params=pltpu.CompilerParams(vmem_limit_bytes=16 * MIB),
        cost_estimate=pl.CostEstimate(
            flops=2 * tokens * depth * width, bytes_accessed=4 * depth * width, transcendentals=0
        ),
        name="forward",
    )(*across, x_near, g_across, g_near, even, odd)


def gradient_kernel(xt, s, grad):
    grad[...] = jnp.dot(xt[...], s[...], preferred_element_type=F32)


def gradient(transposed, slopes):
    depth, tokens = transposed.shape
    width = slopes.shape[1]
    return pl.pallas_call(
        gradient_kernel,
        out_shape=jax.ShapeDtypeStruct((depth, width), F32),
        compiler_params=pltpu.CompilerParams(vmem_limit_bytes=16 * MIB),
        cost_estimate=pl.CostEstimate(
            flops=2 * tokens * depth * width, bytes_accessed=4 * depth * width, transcendentals=0
        ),
        name="gradient",
    )(transposed, slopes)


def finish_kernel(shards, moments, grad, w, *refs):
    given, refs = refs[:moments], refs[moments:]
    home, back, refs = refs[0], refs[1], refs[2:]
    last, (w_out, m_out, v_out, r_out, m, v, w_new, m_new, v_new, r, sem) = refs[:shards], refs[shards:]
    m_even, v_even, m_odd, v_odd, *m_detour = given
    bands = blocks(w.shape[0], 256)
    n = len(bands)
    origin = sources()
    even, odd = lax.rem(origin, 2) == 0, lax.rem(origin, 2) == 1
    m_from, v_from = [(odd, m_odd)], [(even, v_even), (odd, v_odd)]
    if m_detour:
        m_from += [(lax.rem(origin, 4) == 0, m_even), (lax.rem(origin, 4) == 2, m_detour[0])]
    else:
        m_from += [(even, m_even)]
    gets = [
        [
            from_one_of([(when, one.at[band]) for when, one in chosen], ref.at[band], sem.at[5 * i + k])
            for k, (chosen, ref) in enumerate(((m_from, m), (v_from, v)))
        ]
        for i, band in enumerate(bands)
    ]
    total = last[0][...].astype(F32)
    for piece in last[1:]:
        total = total + piece[...].astype(F32)
    r[...] = total.astype(BF16)
    puts = [
        pltpu.make_async_copy(one, r_out.at[i], sem.at[5 * n + i]) for i, one in enumerate((home, back, r))
    ]
    for put in puts:
        put.start()
    for i, band in enumerate(bands):
        for get in gets[i]:
            get.wait()
        update_rows(grad, w, m, v, w_new, m_new, v_new, band)
        new = [
            pltpu.make_async_copy(one.at[band], out.at[band], sem.at[5 * i + 2 + k])
            for k, (one, out) in enumerate(((w_new, w_out), (m_new, m_out), (v_new, v_out)))
        ]
        for put in new:
            put.start()
        puts += new
    for put in puts:
        put.wait()


def finish(grad, kernel, moments, home, back, last):
    depth, width = kernel.shape
    rows = home.shape
    n = len(blocks(depth, 256))
    return pl.pallas_call(
        functools.partial(finish_kernel, len(last), len(moments)),
        out_shape=(
            jax.ShapeDtypeStruct((depth, width), BF16),
            jax.ShapeDtypeStruct((depth, width), F32),
            jax.ShapeDtypeStruct((depth, width), F32),
            jax.ShapeDtypeStruct((HOPS,) + rows, BF16),
        ),
        in_specs=[WHOLE] * 2 + [ANY] * len(moments) + [WHOLE] * (2 + len(last)),
        out_specs=(ANY,) * 4,
        scratch_shapes=[
            pltpu.VMEM((depth, width), BF16),
            pltpu.VMEM((depth, width), BF16),
            pltpu.VMEM((depth, width), BF16),
            pltpu.VMEM((depth, width), F32),
            pltpu.VMEM((depth, width), F32),
            pltpu.VMEM(rows, BF16),
            pltpu.SemaphoreType.DMA((5 * n + HOPS,)),
        ],
        compiler_params=pltpu.CompilerParams(vmem_limit_bytes=24 * MIB),
        cost_estimate=pl.CostEstimate(flops=30 * depth * width, bytes_accessed=16 * depth * width, transcendentals=0),
        name="finish",
    )(grad, kernel, *moments, home, back, *last)


def shards(cut_acts, upstream, weights, moment_one, moment_two):
    kernel, first, second = weights[0], moment_one[0], moment_two[0]
    n, m = lax.axis_size("blk"), lax.axis_size("shard")
    evens, odds = range(0, n, 2), range(1, n, 2)
    share = cut_acts.shape[1] // m
    half = cut(cut_acts, share)
    pairs = n - n % 2
    partner = {i: i ^ 1 if i < pairs else i for i in range(n)}
    neighbour = {i: (i + 1) % n if i % 2 else (i - 1) % n for i in range(n)}
    across = [routed(half, neighbour)]
    across_g = passed_along(upstream, "blk", -1)
    near_x, near_g = routed(cut_acts, partner), routed(upstream, partner)
    kernel1, first1, second1, slopes0 = train([cut_acts], upstream, kernel, first, second, F32)
    across += [passed_along(across[0], "shard", k) for k in range(1, m)]
    before_g = passed_along(upstream, "blk", 1)

    detour = n % 4 == 0
    even_to, odd_to = {i: (i + HOPS) % n for i in evens}, {i: (i + HOPS) % n for i in odds}
    first_to = {i: i - 2 if detour and i % 4 == 2 else to for i, to in even_to.items()}
    odd_to |= {i: partner[i] for i in evens}
    even_to |= {i: partner[i] for i in odds}
    first_to |= {i: i if detour and i % 4 == 1 else partner[i] for i in odds}
    even_w, even_m, even_v, slopes_even = train([near_x], near_g, kernel1, first1, second1, BF16, parity=0)
    even_w = routed(even_w, even_to)
    even_m = routed(even_m, first_to)
    even_v = routed(even_v, even_to)
    odd_w, odd_m, odd_v, slopes_odd = train(across, across_g, kernel1, first1, second1, BF16, parity=1)
    odd_w = routed(odd_w, odd_to)
    odd_m = routed(odd_m, odd_to)
    odd_v = routed(odd_v, odd_to)
    moments = (even_m, even_v, odd_m, odd_v)
    if detour:
        moments += (routed(even_m, {i: (i + 2 + HOPS) % n for i in range(0, n, 4)}),)

    def summed(slopes, kernel):
        parts = [part(slopes, kernel, k) for k in range(1, m)]
        parts = [passed_along(one, "shard", k + 1) for k, one in enumerate(parts)]
        return part(slopes, kernel, 0, parts)

    home = summed([slopes0], kernel)
    back = summed([slopes_even, slopes_odd], kernel1)
    back = passed_along(back, "blk", 1)

    slopes2, moved, transposed = forward(across, near_x, before_g, near_g, even_w, odd_w)
    last = passed_along(summed([slopes2], moved), "blk", -1)
    grad2 = gradient(transposed, slopes2)
    kernel3, first3, second3, returned = finish(grad2, moved, moments, home, back, [last])
    return (kernel3[None], first3[None], second3[None], returned)


def solution(mesh):
    placed = (
        P("blk", None),
        P("blk", "shard"),
        P("blk", None, "shard"),
        P("blk", None, "shard"),
        P("blk", None, "shard"),
    )
    return jax.shard_map(
        shards,
        mesh=mesh,
        in_specs=placed,
        out_specs=(
            P("blk", None, "shard"),
            P("blk", None, "shard"),
            P("blk", None, "shard"),
            P(None, ("blk", "shard"), None),
        ),
        check_vma=False,
    )
```

```python
import functools

import jax
import jax.numpy as jnp
from jax import lax
from jax.experimental import pallas as pl
from jax.experimental.pallas import tpu as pltpu
from jax.sharding import PartitionSpec as P


HOPS = 3
F32, BF16 = jnp.float32, jnp.bfloat16
ANY = pl.BlockSpec(memory_space=pl.ANY)
WHOLE = pl.BlockSpec(memory_space=pltpu.VMEM)
MIB = 1024 * 1024
CUT_FLOPS = 4 * 10**9


def passed_along(part, axis, by):
    devices = lax.axis_size(axis)
    return lax.ppermute(part, axis, [(i, (i + by) % devices) for i in range(devices)])


def routed(part, route):
    return jax.tree.map(lambda one: lax.ppermute(one, "blk", sorted(route.items())), part)


def only_if(chosen, body):
    if chosen is None:
        body()
    else:
        pl.when(chosen)(body)


def gelu_slope(values):
    square = values * values
    tanh_part = jnp.tanh(values * (0.7978845608 + 0.7978845608 * 0.044715 * square))
    return (0.5 + 0.5 * tanh_part) + (values * (1.0 - tanh_part * tanh_part)) * (
        0.5 * 0.7978845608 + 0.5 * 0.7978845608 * 0.134145 * square
    )


def blocks(size, step):
    step = step if size % step == 0 else size
    return [pl.ds(at, step) for at in range(0, size, step)]


def slopes_body(x, g, w, z, s):
    for cols in blocks(g.shape[1], 256):
        z[:, cols] = jnp.dot(x[...], w[:, cols], preferred_element_type=F32)
        for rows in blocks(x.shape[0], 64):
            s[rows, cols] = (g[rows, cols].astype(F32) * gelu_slope(z[rows, cols])).astype(BF16)


def update_rows(grad, w, m, v, w_new, m_new, v_new, rows):
    for at in blocks(rows.size, 32):
        at = pl.ds(rows.start + at.start, at.size)
        gradient = grad[at, :]
        first = 0.9 * m[at, :].astype(F32) + 0.1 * gradient
        second = 0.95 * v[at, :].astype(F32) + 0.05 * (gradient * gradient)
        m_new[at, :] = first.astype(m_new.dtype)
        v_new[at, :] = second.astype(v_new.dtype)
        root = second * lax.rsqrt(second)
        inverse = lax.rsqrt(second + 1e-08 * (2.0 * root + 1e-08))
        w_new[at, :] = (w[at, :].astype(F32) - (0.01 * first) * inverse).astype(BF16)


def copies_of(parts, whole, sems):
    if len(parts) == 1:
        return [pltpu.make_async_copy(parts[0], whole, sems[0])]
    shards = len(parts)
    me = lax.axis_index("shard")
    share = parts[0].shape[1]
    copies = []
    for k, one in enumerate(parts):
        owner = lax.rem(me + (shards - k), shards)
        at = pl.ds(pl.multiple_of(owner * share, share), share)
        copies.append(pltpu.make_async_copy(one, whole.at[:, at], sems[k]))
    return copies


def train_body(fetched, x_in, g_in, w, m, v, w_new, m_new, v_new, s, xt, z, grad, *scratch):
    if fetched:
        x, g, sem = scratch
        gets = copies_of(x_in, x, [sem.at[1 + k] for k in range(len(x_in))])
        gets.append(pltpu.make_async_copy(g_in, g, sem.at[0]))
        for get in gets:
            get.start()
        for get in gets:
            get.wait()
    else:
        x, g = x_in[0], g_in
    xt[...] = x[...].T
    slopes_body(x, g, w, z, s)
    for band in blocks(w.shape[0], 256):
        grad[band, :] = jnp.dot(xt[band, :], s[...], preferred_element_type=F32)
        update_rows(grad, w, m, v, w_new, m_new, v_new, band)


def train(inputs, grad_out, kernel, first, second, out_dtype, parity=None):
    (tokens, width), depth = grad_out.shape, kernel.shape[0]
    k = len(inputs)

    def body(*refs):
        only_if(
            None if parity is None else lax.rem(lax.axis_index("blk"), 2) == parity,
            lambda: train_body(parity is not None, refs[:k], *refs[k:]),
        )

    scratch = [
        pltpu.VMEM((depth, tokens), BF16),
        pltpu.VMEM((tokens, width), F32),
        pltpu.VMEM((depth, width), F32),
    ]
    if parity is not None:
        scratch += [
            pltpu.VMEM((tokens, depth), BF16),
            pltpu.VMEM((tokens, width), BF16),
            pltpu.SemaphoreType.DMA((1 + k,)),
        ]
    return pl.pallas_call(
        body,
        out_shape=(
            jax.ShapeDtypeStruct((depth, width), BF16),
            jax.ShapeDtypeStruct((depth, width), out_dtype),
            jax.ShapeDtypeStruct((depth, width), out_dtype),
            jax.ShapeDtypeStruct((tokens, width), BF16),
        ),
        in_specs=[WHOLE if parity is None else ANY] * (k + 1) + [WHOLE] * 3,
        out_specs=(WHOLE,) * 4,
        scratch_shapes=scratch,
        compiler_params=pltpu.CompilerParams(vmem_limit_bytes=24 * MIB),
        cost_estimate=pl.CostEstimate(
            flops=4 * tokens * depth * width, bytes_accessed=16 * depth * width, transcendentals=0
        ),
    )(*inputs, grad_out, kernel, first, second)


def cut_kernel(x_in, out, sem):
    share = out.shape[1]
    at = pl.multiple_of(lax.axis_index("shard") * share, share)
    get = pltpu.make_async_copy(x_in.at[:, pl.ds(at, share)], out, sem)
    get.start()
    get.wait()


def cut(inputs, share):
    return pl.pallas_call(
        cut_kernel,
        out_shape=jax.ShapeDtypeStruct((inputs.shape[0], share), BF16),
        in_specs=[ANY],
        out_specs=WHOLE,
        scratch_shapes=[pltpu.SemaphoreType.DMA],
        compiler_params=pltpu.CompilerParams(vmem_limit_bytes=8 * MIB),
        cost_estimate=pl.CostEstimate(flops=CUT_FLOPS, bytes_accessed=4 * inputs.size, transcendentals=0),
        name="cut",
    )(inputs)


def part_kernel(shift, n, parities, *refs):
    *given, out = refs
    each = len(given) // len(parities)
    owner = lax.rem(lax.axis_index("shard") + shift, n)
    rows = out.shape[0]
    at = pl.ds(pl.multiple_of(owner * rows, rows), rows)
    for i, parity in enumerate(parities):

        def body(s_in, w_in, *arrived):
            total = lax.dot_general(s_in[at, :], w_in[...], (((1,), (1,)), ((), ())), preferred_element_type=F32)
            for piece in arrived:
                total = total + piece[...].astype(F32)
            out[...] = total.astype(BF16)

        mine = given[i * each : (i + 1) * each]
        chosen = None if parity is None else lax.rem(lax.axis_index("blk"), 2) == parity
        only_if(chosen, functools.partial(body, *mine))


def part(cases, shift):
    n = lax.axis_size("shard")
    slopes, kernel = next(iter(cases.values()))[:2]
    rows, depth = slopes.shape[0] // n, kernel.shape[0]
    return pl.pallas_call(
        functools.partial(part_kernel, shift, n, tuple(cases)),
        out_shape=jax.ShapeDtypeStruct((rows, depth), BF16),
        compiler_params=pltpu.CompilerParams(vmem_limit_bytes=16 * MIB),
        cost_estimate=pl.CostEstimate(flops=2 * rows * kernel.size, bytes_accessed=2 * kernel.size, transcendentals=0),
        name="part",
    )(*[one for case in cases.values() for one in case])


def from_one_of(chosen, dst, sem):
    for condition, src in chosen:
        pl.when(condition)(lambda src=src: pltpu.make_async_copy(src, dst, sem).start())
    return pltpu.make_async_copy(chosen[0][1], dst, sem)


def sources():
    n = lax.axis_size("blk")
    return lax.rem(lax.axis_index("blk") + (n - HOPS % n), n)


def forward_kernel(parity, shards, *refs):
    x_in, (g, w, s, xt, x, z, sem) = refs[:shards], refs[shards:]

    @pl.when(lax.rem(lax.axis_index("blk"), 2) == parity)
    def _():
        gets = copies_of(x_in, x, [sem.at[k] for k in range(shards)])
        for get in gets:
            get.start()
        for get in gets:
            get.wait()
        slopes_body(x, g, w, z, s)
        xt[...] = x[...].T


def forward(inputs, grad_out, kernel, parity):
    (tokens, width), depth = grad_out.shape, kernel.shape[0]
    n = len(inputs)
    return pl.pallas_call(
        functools.partial(forward_kernel, parity, n),
        out_shape=(
            jax.ShapeDtypeStruct((tokens, width), BF16),
            jax.ShapeDtypeStruct((depth, tokens), BF16),
        ),
        in_specs=[ANY] * n + [WHOLE] * 2,
        out_specs=(WHOLE,) * 2,
        scratch_shapes=[
            pltpu.VMEM((tokens, depth), BF16),
            pltpu.VMEM((tokens, width), F32),
            pltpu.SemaphoreType.DMA((n,)),
        ],
        compiler_params=pltpu.CompilerParams(vmem_limit_bytes=16 * MIB),
        cost_estimate=pl.CostEstimate(
            flops=2 * tokens * depth * width, bytes_accessed=4 * depth * width, transcendentals=0
        ),
    )(*inputs, grad_out, kernel)


def gradient_kernel(*refs):
    *given, grad, w = refs
    for parity in range(2):

        def body(s_in, xt_in, w_in):
            grad[...] = jnp.dot(xt_in[...], s_in[...], preferred_element_type=F32)
            w[...] = w_in[...]

        only_if(lax.rem(lax.axis_index("blk"), 2) == parity, functools.partial(body, *given[3 * parity : 3 * parity + 3]))


def gradient(even, odd):
    (depth, tokens), width = even[1].shape, even[0].shape[1]
    return pl.pallas_call(
        gradient_kernel,
        out_shape=(jax.ShapeDtypeStruct((depth, width), F32), jax.ShapeDtypeStruct((depth, width), BF16)),
        compiler_params=pltpu.CompilerParams(vmem_limit_bytes=24 * MIB),
        cost_estimate=pl.CostEstimate(
            flops=2 * tokens * depth * width, bytes_accessed=4 * depth * width, transcendentals=0
        ),
        name="gradient",
    )(*even, *odd)


def finish_kernel(moments, grad, w, *refs):
    given, (w_out, m_out, v_out, m, v, w_new, m_new, v_new, sem) = refs[:moments], refs[moments:]
    m_even, v_even, m_odd, v_odd, *m_detour = given
    bands = blocks(w.shape[0], 256)
    origin = sources()
    even, odd = lax.rem(origin, 2) == 0, lax.rem(origin, 2) == 1
    m_from, v_from = [(odd, m_odd)], [(even, v_even), (odd, v_odd)]
    if m_detour:
        m_from += [(lax.rem(origin, 4) == 0, m_even), (lax.rem(origin, 4) == 2, m_detour[0])]
    else:
        m_from += [(even, m_even)]
    gets = [
        [
            from_one_of([(when, one.at[band]) for when, one in chosen], ref.at[band], sem.at[5 * i + k])
            for k, (chosen, ref) in enumerate(((m_from, m), (v_from, v)))
        ]
        for i, band in enumerate(bands)
    ]
    puts = []
    for i, band in enumerate(bands):
        for get in gets[i]:
            get.wait()
        update_rows(grad, w, m, v, w_new, m_new, v_new, band)
        new = [
            pltpu.make_async_copy(one.at[band], out.at[band], sem.at[5 * i + 2 + k])
            for k, (one, out) in enumerate(((w_new, w_out), (m_new, m_out), (v_new, v_out)))
        ]
        for put in new:
            put.start()
        puts += new
    for put in puts:
        put.wait()


def finish(grad, kernel, moments):
    depth, width = kernel.shape
    n = len(blocks(depth, 256))
    return pl.pallas_call(
        functools.partial(finish_kernel, len(moments)),
        out_shape=(
            jax.ShapeDtypeStruct((depth, width), BF16),
            jax.ShapeDtypeStruct((depth, width), F32),
            jax.ShapeDtypeStruct((depth, width), F32),
        ),
        in_specs=[WHOLE] * 2 + [ANY] * len(moments),
        out_specs=(ANY,) * 3,
        scratch_shapes=[
            pltpu.VMEM((depth, width), BF16),
            pltpu.VMEM((depth, width), BF16),
            pltpu.VMEM((depth, width), BF16),
            pltpu.VMEM((depth, width), F32),
            pltpu.VMEM((depth, width), F32),
            pltpu.SemaphoreType.DMA((5 * n,)),
        ],
        compiler_params=pltpu.CompilerParams(vmem_limit_bytes=24 * MIB),
        cost_estimate=pl.CostEstimate(flops=30 * depth * width, bytes_accessed=16 * depth * width, transcendentals=0),
        name="finish",
    )(grad, kernel, *moments)


def collect_kernel(*refs):
    *returned, out, sem = refs
    puts = [pltpu.make_async_copy(one, out.at[i], sem.at[i]) for i, one in enumerate(returned)]
    for put in puts:
        put.start()
    for put in puts:
        put.wait()


def collect(*returned):
    return pl.pallas_call(
        collect_kernel,
        out_shape=jax.ShapeDtypeStruct((len(returned),) + returned[0].shape, BF16),
        in_specs=[WHOLE] * len(returned),
        out_specs=ANY,
        scratch_shapes=[pltpu.SemaphoreType.DMA((len(returned),))],
        compiler_params=pltpu.CompilerParams(vmem_limit_bytes=8 * MIB),
        cost_estimate=pl.CostEstimate(flops=returned[0].size, bytes_accessed=12 * returned[0].size, transcendentals=0),
        name="collect",
    )(*returned)


def shards(cut_acts, upstream, weights, moment_one, moment_two):
    kernel, first, second = weights[0], moment_one[0], moment_two[0]
    n, m = lax.axis_size("blk"), lax.axis_size("shard")
    evens, odds = range(0, n, 2), range(1, n, 2)
    share = cut_acts.shape[1] // m
    half = cut(cut_acts, share)
    pairs = n - n % 2
    partner = {i: i ^ 1 if i < pairs else i for i in range(n)}
    neighbour = {i: (i + 1) % n if i % 2 else (i - 1) % n for i in range(n)}
    across = [routed(half, neighbour)]
    across_g = passed_along(upstream, "blk", -1)
    near_x, near_g = routed(cut_acts, partner), routed(upstream, partner)
    kernel1, first1, second1, slopes0 = train([cut_acts], upstream, kernel, first, second, F32)
    across += [passed_along(across[0], "shard", k) for k in range(1, m)]
    before_g = passed_along(upstream, "blk", 1)

    detour = n % 4 == 0
    even_to, odd_to = {i: (i + HOPS) % n for i in evens}, {i: (i + HOPS) % n for i in odds}
    first_to = {i: i - 2 if detour and i % 4 == 2 else to for i, to in even_to.items()}
    odd_to |= {i: partner[i] for i in evens}
    even_to |= {i: partner[i] for i in odds}
    first_to |= {i: i if detour and i % 4 == 1 else partner[i] for i in odds}
    even_w, even_m, even_v, slopes_even = train([near_x], near_g, kernel1, first1, second1, BF16, parity=0)
    even_w = routed(even_w, even_to)
    even_m = routed(even_m, first_to)
    even_v = routed(even_v, even_to)
    odd_w, odd_m, odd_v, slopes_odd = train(across, across_g, kernel1, first1, second1, BF16, parity=1)
    odd_w = routed(odd_w, odd_to)
    odd_m = routed(odd_m, odd_to)
    odd_v = routed(odd_v, odd_to)
    moments = (even_m, even_v, odd_m, odd_v)
    if detour:
        moments += (routed(even_m, {i: (i + 2 + HOPS) % n for i in range(0, n, 4)}),)

    def sent(cases, places):
        routes = {k: [(i * m + s, i * m + (s + k) % m) for i in places for s in range(m)] for k in range(1, m)}
        parts = {k: part(cases, k) for k in routes}
        return [lax.ppermute(parts[k], ("blk", "shard"), route) for k, route in routes.items()]

    case0 = {None: (slopes0, kernel)}
    case1 = {0: (slopes_even, kernel1), 1: (slopes_odd, kernel1)}
    arrived0, arrived1 = sent(case0, range(n)), sent(case1, range(n))
    home = part({None: (*case0[None], *arrived0)}, 0)
    back = part({parity: (*case, *arrived1) for parity, case in case1.items()}, 0)
    back = passed_along(back, "blk", 1)

    slopes_o, turned_o = forward([near_x], near_g, even_w, 1)
    arrived_o = sent({1: (slopes_o, even_w)}, odds)
    slopes_e, turned_e = forward(across, before_g, odd_w, 0)
    arrived_e = sent({0: (slopes_e, odd_w)}, evens)
    last = part({0: (slopes_e, odd_w, *arrived_e), 1: (slopes_o, even_w, *arrived_o)}, 0)
    last = passed_along(last, "blk", -1)
    grad2, moved = gradient((slopes_e, turned_e, odd_w), (slopes_o, turned_o, even_w))
    kernel3, first3, second3 = finish(grad2, moved, moments)
    returned = collect(home, back, last)
    return (kernel3[None], first3[None], second3[None], returned)


def solution(mesh):
    placed = (
        P("blk", None),
        P("blk", "shard"),
        P("blk", None, "shard"),
        P("blk", None, "shard"),
        P("blk", None, "shard"),
    )
    return jax.shard_map(
        shards,
        mesh=mesh,
        in_specs=placed,
        out_specs=(
            P("blk", None, "shard"),
            P("blk", None, "shard"),
            P("blk", None, "shard"),
            P(None, ("blk", "shard"), None),
        ),
        check_vma=False,
    )
```
